32 devices in a mesh: grp: 2 (over x), kv: 16 (over z, y, core).
Axes of the slice: x: 2, y: 2, z: 4, core: 2. Of those that a mesh axis runs over, the one named last changes fastest.
Arguments:
- queries: bfloat16 [128, 40, 128], P(('grp', 'kv')), parts along dimension 0, may hold values from -250 to 250
- cache_keys: bfloat16 [8192, 40, 128], P(('grp', 'kv')), parts along dimension 0, may hold values from -8 to 8
- cache_values: bfloat16 [8192, 40, 128], P(('grp', 'kv')), parts along dimension 0, may hold values from -18 to 18
- new_keys: bfloat16 [128, 40, 128], P(('grp', 'kv')), parts along dimension 0, may hold values from -4 to 4
- new_values: bfloat16 [128, 40, 128], P(('grp', 'kv')), parts along dimension 0, may hold values from -4 to 4
- valid_frames: int32 [2], P('grp'), parts along dimension 0, may hold values from 8 to 16
Outputs:
- attended: bfloat16 [128, 40, 128], P(('grp', 'kv')), parts along dimension 0
The draws below stay inside these ranges and needn't reach their ends.
There are 2 independent parts, one for each index of `grp`. The reference program is written for one: setup_inputs(seed, part) draws one part's arguments, and reference() takes and returns one part's arrays. A program takes and returns all parts, laid end to end along the dimension named above; each array names one. Nothing has to cross between parts.
All inputs are finite; a program needn't handle non-finite values.
Results may differ from the reference program's by a relative error of at most 0.0027.
Values may be sent and summed in bfloat16 or wider, within the bound.
A program may use at most 128 MiB of HBM per device.

```python
import math
import jax
import jax.numpy as jnp
from jax import lax

HEADS = 40
HEAD_DIM = 128
FRAME = 256
NEW = 64
CACHE = 4096
FRAMES = 16


def drawn_pair(key):
    base = jax.random.fold_in(key, 11)
    keys_all = jax.random.truncated_normal(jax.random.fold_in(base, 1), -4.0, 4.0, (CACHE, HEADS, HEAD_DIM), jnp.float32)
    query_all = 4.0 * jax.random.truncated_normal(jax.random.fold_in(base, 2), -4.0, 4.0, (NEW, HEADS, HEAD_DIM), jnp.float32)
    return (query_all, keys_all)


def draw_queries(key, part):
    return drawn_pair(key)[0].astype(jnp.bfloat16)


def draw_cache_keys(key, part):
    return drawn_pair(key)[1].astype(jnp.bfloat16)


def draw_cache_values(key, part):
    base = jax.random.fold_in(key, 23)
    values_all = jax.random.truncated_normal(jax.random.fold_in(base, 1), -4.0, 4.0, (CACHE, HEADS, HEAD_DIM), jnp.float32)
    return values_all.astype(jnp.bfloat16)


def shard_levels(own_key, dims, pieces, smallest, largest):
    def one(axis_at, blocks):
        draws = jax.random.uniform(jax.random.fold_in(jax.random.fold_in(own_key, 6), axis_at), (blocks,), jnp.float32, smallest / len(pieces), largest / len(pieces))
        return jnp.repeat(jnp.exp(draws), dims[axis_at] // blocks).reshape((-1,) + (1,) * (len(dims) - axis_at - 1))

    factor_of = one(*pieces[0])
    for cut in pieces[1:]:
        factor_of = factor_of * one(*cut)
    return factor_of


def noise(key, dims, deviation, reach, shards=(), kind=jnp.bfloat16):
    level = shard_levels(key, dims, shards, -0.22, 0.18) if shards else 1.0
    array = jax.random.normal(key, dims, jnp.float32) * deviation * level
    return jnp.minimum(jnp.maximum(array, -reach), reach).astype(kind)


def setup_inputs(seed: int = 0, part: int = 0) -> dict:
    arg_keys = jax.random.split(jax.random.key(seed), 7)
    part_keys = jax.random.split(jax.random.fold_in(arg_keys[6], part), 7)
    return {
        "queries": draw_queries(jax.random.fold_in(jax.random.fold_in(arg_keys[6], part), 71), part),
        "cache_keys": draw_cache_keys(jax.random.fold_in(jax.random.fold_in(arg_keys[6], part), 71), part),
        "cache_values": draw_cache_values(jax.random.fold_in(jax.random.fold_in(arg_keys[6], part), 71), part),
        "new_keys": noise(part_keys[3], (NEW, HEADS, HEAD_DIM), 1.0, 4.0, ((0, 16),)),
        "new_values": noise(part_keys[4], (NEW, HEADS, HEAD_DIM), 1.0, 4.0, ((0, 16),)),
        "valid_frames": jax.random.randint(part_keys[5], (1,), FRAMES // 2, FRAMES + 1).astype(jnp.int32),
    }


def reference(queries, cache_keys, cache_values, new_keys, new_values, valid_frames):
    limit = valid_frames[0] * FRAME
    positions = jnp.arange(CACHE, dtype=jnp.int32)
    live = positions < limit
    factor = 1.0 / math.sqrt(HEAD_DIM)

    def one_head(head):
        query_h = lax.dynamic_index_in_dim(queries, head, 1, keepdims=False)
        ckey_h = lax.dynamic_index_in_dim(cache_keys, head, 1, keepdims=False)
        cval_h = lax.dynamic_index_in_dim(cache_values, head, 1, keepdims=False)
        nkey_h = lax.dynamic_index_in_dim(new_keys, head, 1, keepdims=False)
        nval_h = lax.dynamic_index_in_dim(new_values, head, 1, keepdims=False)
        cache_score = jnp.dot(query_h, ckey_h.T, preferred_element_type=jnp.float32) * factor
        cache_score = jnp.where(live[None, :], cache_score, jnp.float32(-1e+30))
        new_score = jnp.dot(query_h, nkey_h.T, preferred_element_type=jnp.float32) * factor
        top = jnp.maximum(lax.optimization_barrier(jnp.max(cache_score, axis=1)), lax.optimization_barrier(jnp.max(new_score, axis=1)))
        cache_weight = jnp.exp(cache_score - top[:, None])
        new_weight = jnp.exp(new_score - top[:, None])
        total = lax.optimization_barrier(jnp.sum(cache_weight, axis=1)) + lax.optimization_barrier(jnp.sum(new_weight, axis=1))
        numerator = jnp.dot(cache_weight.astype(jnp.bfloat16), cval_h, preferred_element_type=jnp.float32)
        numerator = numerator + jnp.dot(new_weight.astype(jnp.bfloat16), nval_h, preferred_element_type=jnp.float32)
        return (numerator / total[:, None]).astype(jnp.bfloat16)
    result = lax.map(one_head, jnp.arange(HEADS, dtype=jnp.int32))
    return jnp.transpose(result, (1, 0, 2))
```

```python
import functools
import math

import jax
import jax.numpy as jnp
from jax import lax
from jax.experimental import pallas as pl
from jax.experimental.pallas import tpu as pltpu
from jax.sharding import PartitionSpec as P

FRAME = 256
GROUP = 8
LANES = 128
MESH = pl.DeviceIdType.MESH
masked_score = -1e30
F32 = jnp.float32


def round_up(value, unit):
    return (value + unit - 1) // unit * unit


def plane_of(devices):
    chips = devices // 2
    inner = 1
    while (inner * 2) * (inner * 2) <= chips:
        inner *= 2
    return chips // inner, inner


def body(dims, q_ref, ck_ref, cv_ref, nk_ref, nv_ref, vf_ref, out_ref,
         qg, qtmp, kst, vst, tmp, kh, vh, scores, mx, num, crecv, ysum, yrecv, zbuf, zrecv,
         load_sem, q_send, q_recv, mx_send, mx_recv, c_send, c_recv, y_send, y_recv, z_send, z_recv):
    n, outer, inner, groups, q_dev, cache_dev, new_dev, unroll = dims
    rows = n * q_dev
    half = rows // 2
    per_y = half // inner
    keys = kh.shape[1]
    me = lax.axis_index("kv")
    c = lax.rem(me, 2)
    b = lax.rem(me // 2, inner)
    a = me // (2 * inner)

    def index_of(a_at, b_at, c_at):
        return (a_at * inner + b_at) * 2 + c_at

    def slot_of(a_at, b_at, c_at):
        return (c_at * inner + b_at) * outer + a_at

    def turn(base, step, size):
        return lax.rem(base + step, size)

    def remote(src, dst, send, recv, target):
        return pltpu.make_async_remote_copy(
            src_ref=src, dst_ref=dst, send_sem=send, recv_sem=recv,
            device_id={"kv": target}, device_id_type=MESH)

    loads = []
    for g in range(groups):
        for at, (source, target) in enumerate(((ck_ref, kst), (cv_ref, vst))):
            copy = pltpu.make_async_copy(source.at[:, g], target.at[g], load_sem.at[g, at])
            copy.start()
            loads.append(copy)

    barrier = pltpu.get_barrier_semaphore()
    for step in range(1, n):
        pl.semaphore_signal(barrier, inc=1, device_id={"kv": turn(me, step, n)}, device_id_type=MESH)
    pl.semaphore_wait(barrier, n - 1)

    mine = slot_of(a, b, c)
    sent = []

    def push(source, slot, send_at, target):
        copy = remote(source, qg.at[slot], q_send.at[send_at], q_recv.at[slot], target)
        copy.start()
        sent.append(copy)

    def arrived(slot):
        remote(q_ref, qg.at[slot], q_send.at[0], q_recv.at[slot], me).wait_recv()

    inner_base = outer
    core_base = inner_base + outer * inner
    for da in range(1, outer):
        push(q_ref, mine, da, index_of(turn(a, da, outer), b, c))
    for db in range(1, inner):
        push(q_ref, mine, inner_base + db, index_of(a, turn(b, db, inner), c))
    push(q_ref, mine, core_base, index_of(a, b, 1 - c))
    qg[mine] = q_ref[...]

    def relayout(source, fresh, target, g):
        fill = keys - cache_dev - new_dev
        tmp[0 : cache_dev * GROUP] = source[g].astype(F32).reshape(cache_dev * GROUP, LANES)
        tmp[cache_dev * GROUP : (cache_dev + new_dev) * GROUP] = (
            fresh[:, g].astype(F32).reshape(new_dev * GROUP, LANES))
        tmp[(cache_dev + new_dev) * GROUP :] = jnp.zeros((fill * GROUP, LANES), F32)
        for h in range(GROUP):
            target[g * GROUP + h] = tmp[pl.ds(h, keys, stride=GROUP), :].astype(jnp.bfloat16)

    for g in range(groups):
        loads[2 * g].wait()
        relayout(kst, nk_ref, kh, g)

    for da in range(1, outer):
        slot = slot_of(turn(a, da, outer), b, c)
        arrived(slot)
        for db in range(1, inner):
            push(qg.at[slot], slot, inner_base + da * inner + db, index_of(a, turn(b, db, inner), c))
        push(qg.at[slot], slot, core_base + da * inner, index_of(a, b, 1 - c))
    for da in range(outer):
        for db in range(1, inner):
            slot = slot_of(turn(a, da, outer), turn(b, db, inner), c)
            arrived(slot)
            push(qg.at[slot], slot, core_base + da * inner + db, index_of(a, b, 1 - c))

    for g in range(groups):
        loads[2 * g + 1].wait()
        relayout(vst, nv_ref, vh, g)

    for da in range(outer):
        for db in range(inner):
            arrived(slot_of(turn(a, da, outer), turn(b, db, inner), 1 - c))

    factor = 1.0 / math.sqrt(LANES)
    lane = lax.broadcasted_iota(jnp.int32, (rows, LANES), 1)
    key_at = lax.broadcasted_iota(jnp.int32, (rows, keys), 1)
    bound = vf_ref[0] * FRAME - me * cache_dev
    live = jnp.logical_or(
        jnp.logical_and(key_at < cache_dev, key_at < bound),
        jnp.logical_and(key_at >= cache_dev, key_at < cache_dev + new_dev))
    wide = mx.shape[3]

    def score_phase(g):
        qtmp[...] = qg[:, :, g].astype(F32).reshape(rows * GROUP, LANES)

        def head(h, best):
            query = qtmp[pl.ds(h, rows, stride=GROUP), :].astype(jnp.bfloat16)
            score = lax.dot_general(
                query, kh[g * GROUP + h], (((1,), (1,)), ((), ())), preferred_element_type=F32) * factor
            score = jnp.where(live, score, F32(masked_score))
            scores[g * GROUP + h] = score
            return jnp.where(lane == h, jnp.max(score, axis=1, keepdims=True), best)

        best = lax.fori_loop(0, GROUP, head, jnp.zeros((rows, LANES), F32), unroll=unroll)
        if wide > rows:
            best = jnp.concatenate([best, jnp.zeros((wide - rows, LANES), F32)], axis=0)
        mx[g, me] = best.T[0:GROUP]
        for step in range(1, n):
            copy = remote(mx.at[g, me], mx.at[g, me], mx_send.at[g, step], mx_recv.at[g, n - step],
                          turn(me, step, n))
            copy.start()
            sent.append(copy)

    def weight_phase(g):
        for step in range(1, n):
            source = turn(me, step, n)
            remote(mx.at[g, me], mx.at[g, source], mx_send.at[g, 0], mx_recv.at[g, step], me).wait_recv()
        top = jnp.max(mx[g], axis=0)
        top = jnp.concatenate([top, jnp.zeros((LANES - GROUP, wide), F32)], axis=0).T[0:rows]

        def head(h, sums):
            column = jnp.max(jnp.where(lane == h, top, -jnp.inf), axis=1, keepdims=True)
            weight = jnp.exp(scores[g * GROUP + h] - column)
            num[g, h] = jnp.dot(weight.astype(jnp.bfloat16), vh[g * GROUP + h], preferred_element_type=F32)
            return jnp.where(lane == h, jnp.sum(weight, axis=1, keepdims=True), sums)

        num[g, GROUP] = lax.fori_loop(0, GROUP, head, jnp.zeros((rows, LANES), F32), unroll=unroll)
        other = pl.ds(pl.multiple_of((1 - c) * half, 8), half)
        copy = remote(num.at[g, :, other], crecv.at[g], c_send.at[g], c_recv.at[g], index_of(a, b, 1 - c))
        copy.start()
        sent.append(copy)

    def core_phase(g):
        remote(crecv.at[g], crecv.at[g], c_send.at[g], c_recv.at[g], me).wait_recv()
        own = pl.ds(pl.multiple_of(c * half, 8), half)
        ysum[g] = num[g, :, own] + crecv[g]
        for db in range(1, inner):
            b_at = turn(b, db, inner)
            part = pl.ds(pl.multiple_of(b_at * per_y, 8), per_y)
            copy = remote(ysum.at[g, :, part], yrecv.at[g, inner - db], y_send.at[g, db],
                          y_recv.at[g, inner - db], index_of(a, b_at, c))
            copy.start()
            sent.append(copy)

    def inner_phase(g):
        part = pl.ds(pl.multiple_of(b * per_y, 8), per_y)
        total = ysum[g, :, part]
        for db in range(1, inner):
            remote(yrecv.at[g, db], yrecv.at[g, db], y_send.at[g, db], y_recv.at[g, db], me).wait_recv()
            total = total + yrecv[g, db]
        for at in range(outer):
            zbuf[g, at] = total[:, at * q_dev : (at + 1) * q_dev]
        for da in range(1, outer):
            a_at = turn(a, da, outer)
            copy = remote(zbuf.at[g, a_at], zrecv.at[g, outer - da], z_send.at[g, da],
                          z_recv.at[g, outer - da], index_of(a_at, b, c))
            copy.start()
            sent.append(copy)

    def outer_phase(g):
        total = zbuf[g, a]
        for da in range(1, outer):
            remote(zrecv.at[g, da], zrecv.at[g, da], z_send.at[g, da], z_recv.at[g, da], me).wait_recv()
            total = total + zrecv[g, da]
        for h in range(GROUP):
            out_ref[g, h] = total[h] / total[GROUP][:, h : h + 1]

    for g in range(groups):
        score_phase(g)
    stages = (weight_phase, core_phase, inner_phase, outer_phase)
    for step in range(groups + len(stages) - 1):
        for depth, stage in enumerate(stages):
            if 0 <= step - depth < groups:
                stage(step - depth)
    for copy in sent:
        copy.wait_send()


def attend(number, queries, cache_keys, cache_values, new_keys, new_values, valid_frames):
    n = lax.axis_size("kv")
    outer, inner = plane_of(n)
    q_dev, groups = queries.shape[:2]
    cache_dev, new_dev = cache_keys.shape[0], new_keys.shape[0]
    rows = n * q_dev
    half = rows // 2
    per_y = half // inner
    keys = cache_dev + round_up(new_dev, 16)
    slots = GROUP + 1
    wide = round_up(rows, LANES)
    unroll = GROUP if rows <= LANES else 1
    dims = (n, outer, inner, groups, q_dev, cache_dev, new_dev, unroll)
    bf16 = jnp.bfloat16
    vmem = pl.BlockSpec(memory_space=pltpu.VMEM)
    hbm = pl.BlockSpec(memory_space=pl.ANY)
    dma = pltpu.SemaphoreType.DMA
    return pl.pallas_call(
        functools.partial(body, dims),
        out_shape=jax.ShapeDtypeStruct((groups, GROUP, q_dev, LANES), F32),
        in_specs=[vmem, hbm, hbm, vmem, vmem, pl.BlockSpec(memory_space=pltpu.SMEM)],
        out_specs=vmem,
        scratch_shapes=[
            pltpu.VMEM((n, q_dev, groups, GROUP, LANES), bf16),
            pltpu.VMEM((rows * GROUP, LANES), F32),
            pltpu.VMEM((groups, cache_dev, GROUP, LANES), bf16),
            pltpu.VMEM((groups, cache_dev, GROUP, LANES), bf16),
            pltpu.VMEM((keys * GROUP, LANES), F32),
            pltpu.VMEM((groups * GROUP, keys, LANES), bf16),
            pltpu.VMEM((groups * GROUP, keys, LANES), bf16),
            pltpu.VMEM((groups * GROUP, rows, keys), F32),
            pltpu.VMEM((groups, n, GROUP, wide), F32),
            pltpu.VMEM((groups, slots, rows, LANES), F32),
            pltpu.VMEM((groups, slots, half, LANES), F32),
            pltpu.VMEM((groups, slots, half, LANES), F32),
            pltpu.VMEM((groups, inner, slots, per_y, LANES), F32),
            pltpu.VMEM((groups, outer, slots, q_dev, LANES), F32),
            pltpu.VMEM((groups, outer, slots, q_dev, LANES), F32),
            dma((groups, 2)),
            dma((outer + 2 * outer * inner,)),
            dma((n,)),
            dma((groups, n)),
            dma((groups, n)),
            dma((groups,)),
            dma((groups,)),
            dma((groups, inner)),
            dma((groups, inner)),
            dma((groups, outer)),
            dma((groups, outer)),
        ],
        compiler_params=pltpu.CompilerParams(
            collective_id=number, has_side_effects=True, vmem_limit_bytes=62 * 1024 * 1024),
    )(queries, cache_keys, cache_values, new_keys, new_values, valid_frames)


def per_device(queries, cache_keys, cache_values, new_keys, new_values, valid_frames):
    q_dev, heads, head_dim = queries.shape
    groups = heads // GROUP
    arrays = [x.reshape(x.shape[0], groups, GROUP, head_dim)
              for x in (queries, cache_keys, cache_values, new_keys, new_values)]
    calls = 1 if lax.axis_size("kv") * q_dev <= LANES else groups
    size = groups // calls
    parts = [
        attend(at, *[x[:, at * size : (at + 1) * size] for x in arrays], valid_frames)
        for at in range(calls)
    ]
    result = parts[0] if calls == 1 else jnp.concatenate(parts, axis=0)
    return result.transpose(2, 0, 1, 3).reshape(q_dev, heads, head_dim).astype(queries.dtype)


def solution(mesh):
    placed = (P(("grp", "kv"), None, None),) * 5 + (P("grp"),)
    return jax.shard_map(
        per_device,
        mesh=mesh,
        in_specs=placed,
        out_specs=P(("grp", "kv"), None, None),
        check_vma=False,
    )
```

```python
import functools
import math

import jax
import jax.numpy as jnp
from jax import lax
from jax.experimental import pallas as pl
from jax.experimental.pallas import tpu as pltpu
from jax.sharding import PartitionSpec as P

FRAME = 256
GROUP = 8
LOADS = 4
LAGS = (0, 1, 4, 8)
LANES = 128
MESH = pl.DeviceIdType.MESH
masked_score = -1e30
F32 = jnp.float32


def round_up(value, unit):
    return (value + unit - 1) // unit * unit


def plane_of(devices):
    chips = devices // 2
    inner = 1
    while (inner * 2) * (inner * 2) <= chips:
        inner *= 2
    return chips // inner, inner


def body(dims, q_hbm, ck_ref, cv_ref, nk_hbm, nv_hbm, vf_hbm, out_ref,
         q_ref, nk_ref, nv_ref, vf_ref, small_sem,
         qg, qtmp, kst, vst, tmp, kh, vh, scores, mx, num, crecv, ysum, yrecv, zbuf, zrecv,
         load_sem, q_send, q_recv, mx_send, mx_recv, c_send, c_recv, y_send, y_recv, z_send, z_recv):
    n, outer, inner, cuts, q_dev, cache_dev, new_dev, unroll, pack = dims
    groups = cuts[-1]
    rows = n * q_dev
    half = rows // 2
    per_y = half // inner
    keys = kh.shape[1]
    me = lax.axis_index("kv")
    c = lax.rem(me, 2)
    b = lax.rem(me // 2, inner)
    a = me // (2 * inner)

    def index_of(a_at, b_at, c_at):
        return (a_at * inner + b_at) * 2 + c_at

    def slot_of(a_at, b_at, c_at):
        return (c_at * inner + b_at) * outer + a_at

    def turn(base, step, size):
        return lax.rem(base + step, size)

    def remote(src, dst, send, recv, target):
        return pltpu.make_async_remote_copy(
            src_ref=src, dst_ref=dst, send_sem=send, recv_sem=recv,
            device_id={"kv": target}, device_id_type=MESH)

    small = [
        pltpu.make_async_copy(source, target, small_sem.at[at])
        for at, (source, target) in enumerate(
            ((q_hbm, q_ref), (nk_hbm, nk_ref), (nv_hbm, nv_ref), (vf_hbm, vf_ref)))
    ]
    for copy in small:
        copy.start()
    loads = []
    for at, (source, target) in enumerate(((ck_ref, kst), (cv_ref, vst))):
        for part in range(LOADS):
            span = pl.ds(part * (cache_dev // LOADS), cache_dev // LOADS)
            copy = pltpu.make_async_copy(source.at[span], target.at[span], load_sem.at[at, part])
            copy.start()
            loads.append(copy)

    barrier = pltpu.get_barrier_semaphore()
    partners = [index_of(turn(a, da, outer), b, c) for da in range(1, outer)]
    partners += [index_of(a, turn(b, db, inner), c) for db in range(1, inner)]
    partners.append(index_of(a, b, 1 - c))
    for partner in partners:
        pl.semaphore_signal(barrier, inc=1, device_id={"kv": partner}, device_id_type=MESH)
    pl.semaphore_wait(barrier, len(partners))
    small[0].wait()

    mine = slot_of(a, b, c)
    sent = []

    def push(source, slot, piece, send_at, target):
        span = pl.ds(cuts[piece], cuts[piece + 1] - cuts[piece])
        copy = remote(source.at[:, span], qg.at[slot, :, span], q_send.at[piece, send_at],
                      q_recv.at[piece, slot], target)
        copy.start()
        sent.append(copy)

    def arrived(slot, piece):
        span = pl.ds(cuts[piece], cuts[piece + 1] - cuts[piece])
        remote(q_ref.at[:, span], qg.at[slot, :, span], q_send.at[piece, 0], q_recv.at[piece, slot],
               me).wait_recv()

    inner_base = outer
    core_base = inner_base + outer * inner
    pieces = len(cuts) - 1
    for piece in range(pieces):
        for da in range(1, outer):
            push(q_ref, mine, piece, da, index_of(turn(a, da, outer), b, c))
        for db in range(1, inner):
            push(q_ref, mine, piece, inner_base + db, index_of(a, turn(b, db, inner), c))
        push(q_ref, mine, piece, core_base, index_of(a, b, 1 - c))
    qg[mine] = q_ref[...]

    def relayout(source, fresh, target, g):
        fill = keys - cache_dev - new_dev
        tmp[0 : cache_dev * GROUP] = source[:, g].astype(F32).reshape(cache_dev * GROUP, LANES)
        tmp[cache_dev * GROUP : (cache_dev + new_dev) * GROUP] = (
            fresh[:, g].astype(F32).reshape(new_dev * GROUP, LANES))
        tmp[(cache_dev + new_dev) * GROUP :] = jnp.zeros((fill * GROUP, LANES), F32)
        for h in range(GROUP):
            target[g * GROUP + h] = tmp[pl.ds(h, keys, stride=GROUP), :].astype(jnp.bfloat16)

    for copy in small[1:] + loads[:LOADS]:
        copy.wait()
    for g in range(groups):
        relayout(kst, nk_ref, kh, g)

    def forward_outer(piece):
        for da in range(1, outer):
            slot = slot_of(turn(a, da, outer), b, c)
            arrived(slot, piece)
            for db in range(1, inner):
                push(qg.at[slot], slot, piece, inner_base + da * inner + db,
                     index_of(a, turn(b, db, inner), c))
            push(qg.at[slot], slot, piece, core_base + da * inner, index_of(a, b, 1 - c))

    def forward_inner(piece):
        for da in range(outer):
            for db in range(1, inner):
                slot = slot_of(turn(a, da, outer), turn(b, db, inner), c)
                arrived(slot, piece)
                push(qg.at[slot], slot, piece, core_base + da * inner + db, index_of(a, b, 1 - c))

    def gathered(piece):
        for da in range(outer):
            for db in range(inner):
                arrived(slot_of(turn(a, da, outer), turn(b, db, inner), 1 - c), piece)

    factor = 1.0 / math.sqrt(LANES)
    lane = lax.broadcasted_iota(jnp.int32, (rows, LANES), 1)
    key_at = lax.broadcasted_iota(jnp.int32, (rows, keys), 1)
    bound = vf_ref[0] * FRAME - me * cache_dev
    live = jnp.logical_or(
        jnp.logical_and(key_at < cache_dev, key_at < bound),
        jnp.logical_and(key_at >= cache_dev, key_at < cache_dev + new_dev))
    tall, wide = mx.shape[2:]

    def score_phase(g):
        qtmp[...] = qg[:, :, g].astype(F32).reshape(rows * GROUP, LANES)

        def head(h, best):
            query = qtmp[pl.ds(h, rows, stride=GROUP), :].astype(jnp.bfloat16)
            score = lax.dot_general(
                query, kh[g * GROUP + h], (((1,), (1,)), ((), ())), preferred_element_type=F32) * factor
            score = jnp.where(live, score, F32(masked_score))
            scores[g * GROUP + h] = score
            return jnp.where(lane == h, jnp.max(score, axis=1, keepdims=True), best)

        best = lax.fori_loop(0, GROUP, head, jnp.zeros((rows, LANES), F32), unroll=unroll)
        if pack > 1:
            best = jnp.concatenate(
                [best] + [pltpu.roll(best, LANES - at * tall, 1) for at in range(1, pack)], axis=0)
        mx[g, me] = best.T[0:tall]
        for step in range(1, n):
            copy = remote(mx.at[g, me], mx.at[g, me], mx_send.at[g, step], mx_recv.at[g, n - step],
                          turn(me, step, n))
            copy.start()
            sent.append(copy)

    totals = [jnp.zeros((rows, LANES), F32)]
    finished = []

    def slots_of(g):
        return pl.ds(0, GROUP + (g == groups - 1))

    def weight_phase(g):
        for step in range(1, n):
            source = turn(me, step, n)
            remote(mx.at[g, me], mx.at[g, source], mx_send.at[g, 0], mx_recv.at[g, step], me).wait_recv()
        top = jnp.max(mx[g], axis=0)
        turned = jnp.concatenate([top, jnp.zeros((LANES - tall, wide), F32)], axis=0).T
        top = turned[0:rows]
        for at in range(1, pack):
            moved = pltpu.roll(turned[at * rows : (at + 1) * rows], at * tall, 1)
            top = jnp.where(lane < at * tall, top, moved)

        def head(h, sums):
            column = jnp.max(jnp.where(lane == h, top, -jnp.inf), axis=1, keepdims=True)
            weight = jnp.exp(scores[g * GROUP + h] - column)
            num[g, h] = jnp.dot(weight.astype(jnp.bfloat16), vh[g * GROUP + h], preferred_element_type=F32)
            return jnp.where(lane == g * GROUP + h, jnp.sum(weight, axis=1, keepdims=True), sums)

        sums = lax.fori_loop(0, GROUP, head, totals[-1], unroll=unroll)
        totals.append(sums)
        if g == groups - 1:
            num[g, GROUP] = sums
        other = pl.ds(pl.multiple_of((1 - c) * half, 8), half)
        copy = remote(num.at[g, slots_of(g), other], crecv.at[g, slots_of(g)], c_send.at[g], c_recv.at[g], index_of(a, b, 1 - c))
        copy.start()
        sent.append(copy)

    def core_phase(g):
        remote(crecv.at[g, slots_of(g)], crecv.at[g, slots_of(g)], c_send.at[g], c_recv.at[g], me).wait_recv()
        own = pl.ds(pl.multiple_of(c * half, 8), half)
        use = slots_of(g)
        ysum[g, use] = num[g, use, own] + crecv[g, use]
        for db in range(1, inner):
            b_at = turn(b, db, inner)
            part = pl.ds(pl.multiple_of(b_at * per_y, 8), per_y)
            copy = remote(ysum.at[g, use, part], yrecv.at[g, inner - db, use], y_send.at[g, db],
                          y_recv.at[g, inner - db], index_of(a, b_at, c))
            copy.start()
            sent.append(copy)

    def inner_phase(g):
        part = pl.ds(pl.multiple_of(b * per_y, 8), per_y)
        use = slots_of(g)
        total = ysum[g, use, part]
        for db in range(1, inner):
            remote(yrecv.at[g, db, use], yrecv.at[g, db, use], y_send.at[g, db], y_recv.at[g, db], me).wait_recv()
            total = total + yrecv[g, db, use]
        for at in range(outer):
            zbuf[g, at, use] = total[:, at * q_dev : (at + 1) * q_dev]
        for da in range(1, outer):
            a_at = turn(a, da, outer)
            copy = remote(zbuf.at[g, a_at, use], zrecv.at[g, outer - da, use], z_send.at[g, da],
                          z_recv.at[g, outer - da], index_of(a_at, b, c))
            copy.start()
            sent.append(copy)

    def outer_phase(g):
        use = slots_of(g)
        total = zbuf[g, a, use]
        for da in range(1, outer):
            remote(zrecv.at[g, da, use], zrecv.at[g, da, use], z_send.at[g, da], z_recv.at[g, da], me).wait_recv()
            total = total + zrecv[g, da, use]
        finished.append(total)
        if g == groups - 1:
            for done in range(groups):
                for h in range(GROUP):
                    at = done * GROUP + h
                    out_ref[:, done, h] = finished[done][h] / total[GROUP][:, at : at + 1]

    for piece in range(pieces):
        forward_outer(piece)
    for piece in range(pieces):
        forward_inner(piece)
        gathered(piece)
        for g in range(cuts[piece], cuts[piece + 1]):
            score_phase(g)
    for copy in loads[LOADS:]:
        copy.wait()
    for g in range(groups):
        relayout(vst, nv_ref, vh, g)
    stages = (weight_phase, core_phase, inner_phase, outer_phase)
    for step in range(groups + LAGS[-1]):
        for lag, stage in zip(LAGS, stages):
            if 0 <= step - lag < groups:
                stage(step - lag)
    for copy in sent:
        copy.wait_send()


def attend(number, queries, cache_keys, cache_values, new_keys, new_values, valid_frames):
    n = lax.axis_size("kv")
    outer, inner = plane_of(n)
    q_dev, groups = queries.shape[:2]
    cache_dev, new_dev = cache_keys.shape[0], new_keys.shape[0]
    rows = n * q_dev
    half = rows // 2
    per_y = half // inner
    keys = cache_dev + round_up(new_dev, 16)
    slots = GROUP + 1
    wide = max(rows, LANES)
    unroll = GROUP if rows <= LANES else 1
    pack = max(LANES // rows, 1)
    cuts = (0, 2, groups) if groups > 2 else (0, groups)
    pieces = len(cuts) - 1
    dims = (n, outer, inner, cuts, q_dev, cache_dev, new_dev, unroll, pack)
    bf16 = jnp.bfloat16
    vmem = pl.BlockSpec(memory_space=pltpu.VMEM)
    hbm = pl.BlockSpec(memory_space=pl.ANY)
    dma = pltpu.SemaphoreType.DMA
    return pl.pallas_call(
        functools.partial(body, dims),
        out_shape=jax.ShapeDtypeStruct((q_dev, groups, GROUP, LANES), F32),
        in_specs=[hbm] * 6,
        out_specs=vmem,
        scratch_shapes=[
            pltpu.VMEM(queries.shape, bf16),
            pltpu.VMEM(new_keys.shape, bf16),
            pltpu.VMEM(new_values.shape, bf16),
            pltpu.SMEM(valid_frames.shape, jnp.int32),
            dma((4,)),
            pltpu.VMEM((n, q_dev, groups, GROUP, LANES), bf16),
            pltpu.VMEM((rows * GROUP, LANES), F32),
            pltpu.VMEM((cache_dev, groups, GROUP, LANES), bf16),
            pltpu.VMEM((cache_dev, groups, GROUP, LANES), bf16),
            pltpu.VMEM((keys * GROUP, LANES), F32),
            pltpu.VMEM((groups * GROUP, keys, LANES), bf16),
            pltpu.VMEM((groups * GROUP, keys, LANES), bf16),
            pltpu.VMEM((groups * GROUP, rows, keys), F32),
            pltpu.VMEM((groups, n, GROUP // pack, wide), F32),
            pltpu.VMEM((groups, slots, rows, LANES), F32),
            pltpu.VMEM((groups, slots, half, LANES), F32),
            pltpu.VMEM((groups, slots, half, LANES), F32),
            pltpu.VMEM((groups, inner, slots, per_y, LANES), F32),
            pltpu.VMEM((groups, outer, slots, q_dev, LANES), F32),
            pltpu.VMEM((groups, outer, slots, q_dev, LANES), F32),
            dma((2, LOADS)),
            dma((pieces, outer + 2 * outer * inner)),
            dma((pieces, n)),
            dma((groups, n)),
            dma((groups, n)),
            dma((groups,)),
            dma((groups,)),
            dma((groups, inner)),
            dma((groups, inner)),
            dma((groups, outer)),
            dma((groups, outer)),
        ],
        compiler_params=pltpu.CompilerParams(
            collective_id=number, has_side_effects=True, vmem_limit_bytes=62 * 1024 * 1024),
    )(queries, cache_keys, cache_values, new_keys, new_values, valid_frames)


def per_device(queries, cache_keys, cache_values, new_keys, new_values, valid_frames):
    q_dev, heads, head_dim = queries.shape
    groups = heads // GROUP
    arrays = [x.reshape(x.shape[0], groups, GROUP, head_dim)
              for x in (queries, cache_keys, cache_values, new_keys, new_values)]
    calls = 1 if lax.axis_size("kv") * q_dev <= LANES else groups
    size = groups // calls
    parts = [
        attend(at, *[x[:, at * size : (at + 1) * size] for x in arrays], valid_frames)
        for at in range(calls)
    ]
    result = parts[0] if calls == 1 else jnp.concatenate(parts, axis=1)
    return result.reshape(q_dev, heads, head_dim).astype(queries.dtype)


def solution(mesh):
    placed = (P(("grp", "kv"), None, None),) * 5 + (P("grp"),)
    return jax.shard_map(
        per_device,
        mesh=mesh,
        in_specs=placed,
        out_specs=P(("grp", "kv"), None, None),
        check_vma=False,
    )
```
